128 devices in a mesh: gx: 8 (over x_lo, z), gy: 4 (over y), gz: 4 (over x_hi, core).
Axes of the slice: x: 4 (x_hi: 2, x_lo: 2; x = x_hi * 2 + x_lo), y: 4, z: 4, core: 2. Of those that a mesh axis runs over, the one named last changes fastest.
Arguments:
- inputs: bfloat16 [2560, 8192], P(('gx', 'gz'), 'gy'), may hold values from -6 to 6
- out_grad: bfloat16 [2560, 8192], P(('gx', 'gz'), 'gy'), may hold values from -6 to 6
- gate_weight: bfloat16 [8192, 16384], P('gy', ('gx', 'gz')), may hold values from -0.0625 to 0.0625
- up_weight: bfloat16 [8192, 16384], P('gy', ('gx', 'gz')), may hold values from -0.0625 to 0.0625
- down_weight: bfloat16 [16384, 8192], P(('gx', 'gz'), 'gy'), may hold values from -0.046875 to 0.046875
Outputs:
- in_grad: bfloat16 [2560, 8192], P(('gx', 'gz'), 'gy')
The draws below stay inside these ranges and needn't reach their ends.
All inputs are finite; a program needn't handle non-finite values.
Results may differ from the reference program's by a relative error of at most 0.0049.
Values may be sent and summed in bfloat16 or wider, within the bound.
No kernel may reach another device: no remote copies, remote signals or barrier semaphores. Data moves between devices by JAX's collectives and lax.ppermute only.
A program may use at most 128 MiB of HBM per device.

```python
import jax
import jax.numpy as jnp
from jax import lax

D = 8192
FF = 16384
TOKENS = 2560


def shard_levels(rng, shape, split, least, top_value):
    gain = 1.0
    for dim, shards_of in split:
        heights = jax.random.uniform(jax.random.fold_in(jax.random.fold_in(rng, 6), dim), (shards_of,), jnp.float32, least / len(split), top_value / len(split))
        gain = gain * jnp.repeat(jnp.exp(heights), shape[dim] // shards_of).reshape((-1,) + (1,) * (len(shape) - 1 - dim))
    return gain


def bell_draw(key, shape, deviation, bound, pieces=(), held_as=jnp.bfloat16):
    factor_of = shard_levels(key, shape, pieces, -0.22, 0.18) if pieces else 1.0
    result = jax.random.normal(key, shape, jnp.float32) * deviation * factor_of
    return jnp.minimum(jnp.maximum(result, -bound), bound).astype(held_as)


def setup_inputs(seed: int = 0) -> dict:
    arg_keys = jax.random.split(jax.random.key(seed), 6)
    return {
        "inputs": bell_draw(arg_keys[0], (TOKENS, D), 1.0, 6.0, ((0, 32), (1, 4))),
        "out_grad": bell_draw(arg_keys[1], (TOKENS, D), 1.0, 6.0, ((0, 32), (1, 4))),
        "gate_weight": bell_draw(arg_keys[2], (D, FF), D ** -0.5, 0.0625, ((0, 4), (1, 32))),
        "up_weight": bell_draw(arg_keys[3], (D, FF), D ** -0.5, 0.0625, ((0, 4), (1, 32))),
        "down_weight": bell_draw(arg_keys[4], (FF, D), FF ** -0.5, 0.046875, ((0, 32), (1, 4))),
    }


def contract_last(left, right):
    return lax.dot_general(left, right, (((1,), (1,)), ((), ())), preferred_element_type=jnp.float32)


def reference(inputs, out_grad, gate_weight, up_weight, down_weight):
    gate = jnp.dot(inputs, gate_weight, preferred_element_type=jnp.float32)
    upper = jnp.dot(inputs, up_weight, preferred_element_type=jnp.float32)
    hidden_grad = contract_last(out_grad, down_weight)
    logistic = jax.nn.sigmoid(gate)
    gate_grad = (hidden_grad * upper * logistic * (1.0 + gate * (1.0 - logistic))).astype(jnp.bfloat16)
    up_grad = (hidden_grad * gate * logistic).astype(jnp.bfloat16)
    total = contract_last(gate_grad, gate_weight) + contract_last(up_grad, up_weight)
    return total.astype(jnp.bfloat16)
```

```python
import jax
import jax.numpy as jnp
from jax import lax
from jax.sharding import Mesh, PartitionSpec as P

CHUNKS = (40, 40)
RING = 4
XZ = ("xh", "xl", "z")


def place_of(axis):
    if axis == "x":
        return lax.axis_index("xh") * 2 + lax.axis_index("xl")
    return lax.axis_index(axis)


def shift(value, axis, step):
    if axis == "x":
        order = lambda i: (i % 2) * 2 + i // 2
        pairs = [(order(i), order((i + step) % RING)) for i in range(RING)]
        return lax.ppermute(value, ("xl", "xh"), pairs)
    return lax.ppermute(value, axis, [(i, (i + step) % RING) for i in range(RING)])


def gather(value, axis, dim):
    here = place_of(axis)
    shape = value.shape[:dim] + (RING,) + value.shape[dim:]
    filled = jnp.zeros(shape, value.dtype)
    for step in (1, 3, 2, 0):
        piece = value if step == 0 else shift(value, axis, step)
        filled = lax.dynamic_update_index_in_dim(filled, piece, (here - step) % RING, dim)
    return filled


def contract_last(left, right):
    return lax.dot_general(
        left, right, (((1,), (1,)), ((), ())), preferred_element_type=jnp.float32
    )


def exchange_sum(value, axis, members):
    rows, width = value.shape
    blocks = value.reshape(members, rows // members, width)
    return lax.all_to_all(blocks, axis, 0, 0).astype(jnp.float32).sum(axis=0)


def local_grads(gate, upper, hidden_grad):
    logistic = jax.nn.sigmoid(gate)
    gate_grad = (hidden_grad * upper * logistic * (1.0 + gate * (1.0 - logistic))).astype(
        jnp.bfloat16
    )
    up_grad = (hidden_grad * gate * logistic).astype(jnp.bfloat16)
    return jnp.concatenate((gate_grad, up_grad), axis=1)


def shards(inputs, out_grad, gate_weight, up_weight, down_weight):
    swap = [(0, 1), (1, 0)]
    gate_other = lax.ppermute(gate_weight, "core", swap)
    up_other = lax.ppermute(up_weight, "core", swap)
    down_other = lax.ppermute(down_weight, "core", swap)
    both = jnp.concatenate((gate_weight, gate_other, up_weight, up_other), axis=1)
    down = jnp.concatenate((down_weight, down_other), axis=0)
    width = both.shape[0]
    hidden = down.shape[0]
    results = []
    at = 0
    for rows in CHUNKS:
        own_in = lax.slice_in_dim(inputs, at, at + rows)
        own_grad = lax.slice_in_dim(out_grad, at, at + rows)
        at += rows
        rows_in = gather(gather(own_in, "z", 0), "x", 0).reshape(-1, width)
        rows_grad = gather(gather(own_grad, "x", 0), "z", 1).reshape(-1, width)
        pair = jnp.dot(rows_in, both, preferred_element_type=jnp.float32).astype(jnp.bfloat16)
        back = contract_last(rows_grad, down).astype(jnp.bfloat16)
        pair = exchange_sum(pair, "y", RING)
        hidden_grad = exchange_sum(back, "y", RING)
        grads = local_grads(pair[:, :hidden], pair[:, hidden:], hidden_grad)
        grads = gather(grads, "y", 0).reshape(-1, 2 * hidden)
        partial_value = contract_last(grads, both).astype(jnp.bfloat16)
        results.append(exchange_sum(partial_value, XZ, RING * RING).astype(jnp.bfloat16))
    return jnp.concatenate(results, axis=0)


def solution(mesh):
    fine = Mesh(mesh.devices.reshape(2, 4, 4, 2, 2), ("xl", "z", "y", "xh", "core"))
    tokens = ("xl", "z", "xh", "core")
    return jax.shard_map(
        shards,
        mesh=fine,
        in_specs=(P(tokens, "y"), P(tokens, "y"), P("y", tokens), P("y", tokens), P(tokens, "y")),
        out_specs=P(tokens, "y"),
        check_vma=False,
    )
```

```python
import jax
import jax.numpy as jnp
from jax import lax
from jax.experimental import pallas as pl
from jax.experimental.pallas import tpu as pltpu
from jax.sharding import Mesh, PartitionSpec as P

CHUNKS = (40, 40)
RING = 4
XZ = ("xh", "xl", "z")
ORDER = (2, 1, 3, 0)
LAST = (((1,), (1,)), ((), ()))
VMEM_LIMIT = 40 << 20


def place_of(axis):
    if axis == "x":
        return lax.axis_index("xh") * 2 + lax.axis_index("xl")
    return lax.axis_index(axis)


def shift(value, axis, step):
    if axis == "x":
        order = lambda i: (i % 2) * 2 + i // 2
        pairs = [(order(i), order((i + step) % RING)) for i in range(RING)]
        return lax.ppermute(value, ("xl", "xh"), pairs)
    return lax.ppermute(value, axis, [(i, (i + step) % RING) for i in range(RING)])


def gather(value, axis, dim):
    here = place_of(axis)
    shape = value.shape[:dim] + (RING,) + value.shape[dim:]
    filled = jnp.zeros(shape, value.dtype)
    for step in (1, 3, 2, 0):
        piece = value if step == 0 else shift(value, axis, step)
        filled = lax.dynamic_update_index_in_dim(filled, piece, (here - step) % RING, dim)
    return filled


def terms_kernel(place, in_ref, grad_ref, gate_a, gate_b, up_a, up_b, down_a, down_b, *outs):
    step = pl.program_id(0)
    half = outs[0].shape[0]
    cols = jnp.concatenate((gate_a[...], gate_b[...], up_a[...], up_b[...]), axis=1)
    pair = jnp.dot(in_ref[...], cols, preferred_element_type=jnp.float32)
    lines = jnp.concatenate((down_a[...], down_b[...]), axis=0)
    back = lax.dot_general(grad_ref[...], lines, LAST, preferred_element_type=jnp.float32)
    split = pair.shape[1]
    for k in range(RING):

        @pl.when(step == k)
        def _(k=k):
            for side in range(2):
                out = outs[2 * k + side]
                rows = slice(side * half, (side + 1) * half)
                out[:, :split] = pair[rows].astype(out.dtype)
                out[:, split:] = back[rows].astype(out.dtype)


def partial_terms(place, rows_in, rows_grad, gates, ups, downs):
    rows, width = rows_in.shape
    half = rows // 2
    cut = downs[0].shape[0] // RING
    wide = 2 * cut
    bf, f32 = jnp.bfloat16, jnp.float32
    types = (bf, bf, f32, bf, bf, f32, f32, f32)
    act = pl.BlockSpec(memory_space=pltpu.VMEM)
    cols = pl.BlockSpec((width, cut), lambda step, place: (0, place[step]))
    lines = pl.BlockSpec((cut, width), lambda step, place: (place[step], 0))
    grid_spec = pltpu.PrefetchScalarGridSpec(
        num_scalar_prefetch=1,
        grid=(RING,),
        in_specs=[act, act, cols, cols, cols, cols, lines, lines],
        out_specs=[pl.BlockSpec((half, 3 * wide), lambda step, place: (0, 0)) for _ in types],
    )
    return pl.pallas_call(
        terms_kernel,
        grid_spec=grid_spec,
        out_shape=[jax.ShapeDtypeStruct((half, 3 * wide), t) for t in types],
        cost_estimate=pl.CostEstimate(
            flops=2 * rows * width * 12 * wide, bytes_accessed=20 << 20, transcendentals=0
        ),
        compiler_params=pltpu.CompilerParams(vmem_limit_bytes=VMEM_LIMIT),
        name="terms",
    )(place, rows_in, rows_grad, *gates, *ups, *downs)


def back_kernel(place, *rest):
    pieces, cols, out_ref, held = rest[:8], rest[8:12], rest[12], rest[13]
    half = pieces[0].shape[0]
    cut = pieces[0].shape[1] // 4
    span = RING * cut

    @pl.when(pl.program_id(0) == 0)
    def _():
        for k in range(RING):
            at = pl.multiple_of(place[k] * cut, cut)
            for side in range(2):
                for part in range(4):
                    held[side * half : (side + 1) * half, pl.ds(at + part * span, cut)] = pieces[
                        2 * k + side
                    ][:, part * cut : (part + 1) * cut]

    out_ref[...] = lax.dot_general(
        held[...],
        jnp.concatenate([c[...] for c in cols], axis=1),
        LAST,
        preferred_element_type=jnp.float32,
    ).astype(out_ref.dtype)


def back_terms(place, pieces, gates, ups, rows_cut=512):
    half = pieces[0].shape[0]
    width, span = gates[0].shape
    grid_spec = pltpu.PrefetchScalarGridSpec(
        num_scalar_prefetch=1,
        grid=(width // rows_cut,),
        in_specs=[pl.BlockSpec(memory_space=pltpu.VMEM) for _ in pieces]
        + [pl.BlockSpec((rows_cut, span), lambda n, place: (n, 0)) for _ in range(4)],
        out_specs=pl.BlockSpec((2 * half, rows_cut), lambda n, place: (0, n)),
        scratch_shapes=[pltpu.VMEM((2 * half, 4 * span), jnp.bfloat16)],
    )
    return pl.pallas_call(
        back_kernel,
        grid_spec=grid_spec,
        out_shape=jax.ShapeDtypeStruct((2 * half, width), jnp.bfloat16),
        cost_estimate=pl.CostEstimate(
            flops=16 * half * width * span, bytes_accessed=14 << 20, transcendentals=0
        ),
        compiler_params=pltpu.CompilerParams(vmem_limit_bytes=VMEM_LIMIT),
        name="back",
    )(place, *pieces, *gates, *ups)


def narrow(value):
    return value.astype(jnp.bfloat16)


def local_grads(total):
    wide = total.shape[1] // 3
    gate, upper, hidden_grad = total[:, :wide], total[:, wide : 2 * wide], total[:, 2 * wide :]
    logistic = jax.nn.sigmoid(gate)
    gate_grad = hidden_grad * upper * logistic * (1.0 + gate * (1.0 - logistic))
    up_grad = hidden_grad * gate * logistic
    return narrow(jnp.concatenate((gate_grad, up_grad), axis=1))


def first_rows(own_in, own_grad):
    return gather(own_in, "z", 0), gather(own_grad, "x", 0)


def second_rows(some_in, some_grad, width):
    rows_in = gather(some_in, "x", 0).reshape(-1, width)
    return rows_in, gather(some_grad, "z", 1).reshape(-1, width)


def finish(place, terms, gates, ups, rows):
    far_t, far_b, right_t, right_b, left_t, left_b, own_t, own_b = terms
    far_t = shift(far_t, "y", 1)
    far_b = shift(far_b, "y", -1)
    right_b = shift(right_b, "y", 1)
    left_t = shift(left_t, "y", -1)
    right_t = shift(narrow(right_t + far_t), "y", 1)
    left_b = shift(narrow(left_b + far_b), "y", -1)
    top = local_grads(own_t + left_t + right_t)
    low = local_grads(own_b + right_b + left_b)
    from_left_t = shift(top, "y", 1)
    from_right_b = shift(low, "y", -1)
    from_left_b = shift(low, "y", 1)
    from_right_t = shift(top, "y", -1)
    far_top = shift(from_left_t, "y", 1)
    far_low = shift(from_right_b, "y", -1)
    pieces = (far_top, far_low, from_right_t, from_right_b, from_left_t, from_left_b, top, low)
    partial_value = back_terms(place, pieces, gates, ups)
    blocks = partial_value.reshape(RING * RING, rows, -1)
    crossed = lax.all_to_all(blocks, XZ, 0, 0)
    return narrow(crossed.astype(jnp.float32).sum(axis=0))


def swap(value):
    return lax.ppermute(value, "core", [(0, 1), (1, 0)])


def step_shards(inputs, out_grad, gate_weight, up_weight, down_weight):
    gates = (gate_weight, swap(gate_weight))
    ups = (up_weight, swap(up_weight))
    downs = (down_weight, swap(down_weight))
    width = gate_weight.shape[0]
    place = (lax.axis_index("y") + jnp.array(ORDER, jnp.int32)) % RING
    results = []
    at = 0
    some = terms = None
    for rows in CHUNKS:
        own_in = lax.slice_in_dim(inputs, at, at + rows)
        own_grad = lax.slice_in_dim(out_grad, at, at + rows)
        at += rows
        if some is not None:
            own_in, own_grad, *some = lax.optimization_barrier((own_in, own_grad, *some))
            filled = second_rows(*some, width)
            terms = partial_terms(place, *filled, gates, ups, downs)
        some = first_rows(own_in, own_grad)
        if terms is not None:
            *some, terms = lax.optimization_barrier((*some, terms))
            results.append(finish(place, terms, gates, ups, last))
        last = rows
    filled = second_rows(*some, width)
    terms = partial_terms(place, *filled, gates, ups, downs)
    results.append(finish(place, terms, gates, ups, rows))
    return jnp.concatenate(results, axis=0)


def solution(mesh):
    fine = Mesh(mesh.devices.reshape(2, 4, 4, 2, 2), ("xl", "z", "y", "xh", "core"))
    tokens = ("xl", "z", "xh", "core")
    return jax.shard_map(
        step_shards,
        mesh=fine,
        in_specs=(P(tokens, "y"), P(tokens, "y"), P("y", tokens), P("y", tokens), P(tokens, "y")),
        out_specs=P(tokens, "y"),
        check_vma=False,
    )
```

```python
import functools

import jax
import jax.numpy as jnp
from jax import lax
from jax.experimental import pallas as pl
from jax.experimental.pallas import tpu as pltpu
from jax.sharding import Mesh, PartitionSpec as P

CHUNKS = (40, 40)
RING = 4
XZ = ("xh", "xl", "z")
ORDER = (2, 1, 3, 0)
LAST = (((1,), (1,)), ((), ()))
VMEM_LIMIT = 40 << 20


def place_of(axis):
    if axis == "x":
        return lax.axis_index("xh") * 2 + lax.axis_index("xl")
    return lax.axis_index(axis)


def shift(value, axis, step):
    if axis == "x":
        order = lambda i: (i % 2) * 2 + i // 2
        pairs = [(order(i), order((i + step) % RING)) for i in range(RING)]
        return lax.ppermute(value, ("xl", "xh"), pairs)
    return lax.ppermute(value, axis, [(i, (i + step) % RING) for i in range(RING)])


def around(value, axis):
    return [value] + [shift(value, axis, step) for step in range(1, RING)]


def join_kernel(rows, place, *refs):
    pieces, outs = refs[:RING], refs[RING:]
    for k in range(RING):
        at = 0
        for count, out in zip(rows, outs):
            to = pl.multiple_of(place[k] * count, count)
            out[pl.ds(to, count)] = pieces[k][at : at + count]
            at += count


def join(axis, pieces):
    width = pieces[0].shape[1]
    place = (place_of(axis) - jnp.arange(RING, dtype=jnp.int32)) % RING
    spec = pl.BlockSpec(memory_space=pltpu.VMEM)
    return pl.pallas_call(
        functools.partial(join_kernel, CHUNKS),
        in_specs=[pl.BlockSpec(memory_space=pltpu.SMEM)] + [spec] * RING,
        out_specs=[spec] * len(CHUNKS),
        out_shape=[jax.ShapeDtypeStruct((RING * rows, width), pieces[0].dtype) for rows in CHUNKS],
        cost_estimate=pl.CostEstimate(flops=1 << 20, bytes_accessed=3 << 20, transcendentals=0),
        compiler_params=pltpu.CompilerParams(vmem_limit_bytes=16 << 20),
        name="join",
    )(place, *pieces)


def assemble(axis_place, pieces, held):
    count = pieces[0].shape[0]
    for k in range(RING):
        at = pl.multiple_of(axis_place[k] * count, count)
        held[pl.ds(at, count)] = pieces[k][...]


def pair_kernel(place, order, *refs):
    pieces, (gate_a, gate_b, up_a, up_b) = refs[:RING], refs[RING : RING + 4]
    outs, held = refs[RING + 4 : -1], refs[-1]
    step = pl.program_id(0)
    half = outs[0].shape[0]

    @pl.when(step == 0)
    def _():
        assemble(order, pieces, held)

    cols = jnp.concatenate((gate_a[...], gate_b[...], up_a[...], up_b[...]), axis=1)
    pair = jnp.dot(held[...], cols, preferred_element_type=jnp.float32)
    for k in range(RING):

        @pl.when(step == k)
        def _(k=k):
            for side in range(2):
                out = outs[2 * k + side]
                out[...] = pair[side * half : (side + 1) * half].astype(out.dtype)


def pair_terms(place, pieces, gates, ups):
    rows, width = pieces[0].shape[0] * RING, pieces[0].shape[1]
    half = rows // 2
    cut = gates[0].shape[1] // RING
    wide = 2 * cut
    bf, f32 = jnp.bfloat16, jnp.float32
    types = (bf, bf, f32, bf, bf, f32, f32, f32)
    order = (place_of("x") - jnp.arange(RING, dtype=jnp.int32)) % RING
    cols = pl.BlockSpec((width, cut), lambda step, place, order: (0, place[step]))
    grid_spec = pltpu.PrefetchScalarGridSpec(
        num_scalar_prefetch=2,
        grid=(RING,),
        in_specs=[pl.BlockSpec(memory_space=pltpu.VMEM)] * RING + [cols] * 4,
        out_specs=[pl.BlockSpec((half, 2 * wide), lambda *_: (0, 0)) for _ in types],
        scratch_shapes=[pltpu.VMEM((rows, width), bf)],
    )
    return pl.pallas_call(
        pair_kernel,
        grid_spec=grid_spec,
        out_shape=[jax.ShapeDtypeStruct((half, 3 * wide), t) for t in types],
        cost_estimate=pl.CostEstimate(
            flops=2 * rows * width * 8 * wide, bytes_accessed=14 << 20, transcendentals=0
        ),
        compiler_params=pltpu.CompilerParams(vmem_limit_bytes=VMEM_LIMIT),
        name="pair",
    )(place, order, *pieces, *gates, *ups)


def hidden_kernel(place, order, *refs):
    pieces, (down_a, down_b) = refs[:RING], refs[RING : RING + 2]
    outs, held = refs[RING + 2 + 2 * RING : -1], refs[-1]
    step = pl.program_id(0)
    half = outs[0].shape[0]
    count = half // (2 * RING)

    @pl.when(step == 0)
    def _():
        assemble(order, pieces, held)

    lines = jnp.concatenate((down_a[...], down_b[...]), axis=0)
    back = lax.dot_general(held[...], lines, LAST, preferred_element_type=jnp.float32)
    for k in range(RING):

        @pl.when(step == k)
        def _(k=k):
            for x in range(RING):
                out = outs[2 * k + x // 2]
                for z in range(RING):
                    to, at = ((x % 2) * RING + z) * count, (z * RING + x) * count
                    out[to : to + count] = back[at : at + count].astype(out.dtype)


def hidden_terms(place, pieces, downs, terms):
    rows, width = pieces[0].shape[0] * RING, pieces[0].shape[1]
    half = rows // 2
    cut = downs[0].shape[0] // RING
    wide = 2 * cut
    order = (place_of("z") - jnp.arange(RING, dtype=jnp.int32)) % RING
    lines = pl.BlockSpec((cut, width), lambda step, place, order: (place[step], 0))
    grid_spec = pltpu.PrefetchScalarGridSpec(
        num_scalar_prefetch=2,
        grid=(RING,),
        in_specs=[pl.BlockSpec(memory_space=pltpu.VMEM)] * RING
        + [lines, lines]
        + [pl.BlockSpec(memory_space=pl.ANY) for _ in terms],
        out_specs=[pl.BlockSpec((half, wide), lambda *_: (0, 2)) for _ in terms],
        scratch_shapes=[pltpu.VMEM((rows, width), jnp.bfloat16)],
    )
    return pl.pallas_call(
        hidden_kernel,
        grid_spec=grid_spec,
        out_shape=[jax.ShapeDtypeStruct(t.shape, t.dtype) for t in terms],
        input_output_aliases={2 + RING + 2 + k: k for k in range(2 * RING)},
        cost_estimate=pl.CostEstimate(
            flops=2 * rows * width * 4 * wide, bytes_accessed=7 << 20, transcendentals=0
        ),
        compiler_params=pltpu.CompilerParams(vmem_limit_bytes=VMEM_LIMIT),
        name="hidden",
    )(place, order, *pieces, *downs, *terms)


def back_kernel(place, *rest):
    pieces, cols, out_ref, held = rest[:8], rest[8:12], rest[12], rest[13]
    half = pieces[0].shape[0]
    cut = pieces[0].shape[1] // 4
    span = RING * cut

    @pl.when(pl.program_id(0) == 0)
    def _():
        for k in range(RING):
            at = pl.multiple_of(place[k] * cut, cut)
            for side in range(2):
                for part in range(4):
                    held[side * half : (side + 1) * half, pl.ds(at + part * span, cut)] = pieces[
                        2 * k + side
                    ][:, part * cut : (part + 1) * cut]

    out_ref[...] = lax.dot_general(
        held[...],
        jnp.concatenate([c[...] for c in cols], axis=1),
        LAST,
        preferred_element_type=jnp.float32,
    ).astype(out_ref.dtype)


def back_terms(place, pieces, gates, ups, rows_cut=512):
    half = pieces[0].shape[0]
    width, span = gates[0].shape
    grid_spec = pltpu.PrefetchScalarGridSpec(
        num_scalar_prefetch=1,
        grid=(width // rows_cut,),
        in_specs=[pl.BlockSpec(memory_space=pltpu.VMEM) for _ in pieces]
        + [pl.BlockSpec((rows_cut, span), lambda n, place: (n, 0)) for _ in range(4)],
        out_specs=pl.BlockSpec((2 * half, rows_cut), lambda n, place: (0, n)),
        scratch_shapes=[pltpu.VMEM((2 * half, 4 * span), jnp.bfloat16)],
    )
    return pl.pallas_call(
        back_kernel,
        grid_spec=grid_spec,
        out_shape=jax.ShapeDtypeStruct((2 * half, width), jnp.bfloat16),
        cost_estimate=pl.CostEstimate(
            flops=16 * half * width * span, bytes_accessed=14 << 20, transcendentals=0
        ),
        compiler_params=pltpu.CompilerParams(vmem_limit_bytes=VMEM_LIMIT),
        name="back",
    )(place, *pieces, *gates, *ups)


def narrow(value):
    return value.astype(jnp.bfloat16)


def local_grads(total):
    wide = total.shape[1] // 3
    gate, upper, hidden_grad = total[:, :wide], total[:, wide : 2 * wide], total[:, 2 * wide :]
    logistic = jax.nn.sigmoid(gate)
    gate_grad = hidden_grad * upper * logistic * (1.0 + gate * (1.0 - logistic))
    up_grad = hidden_grad * gate * logistic
    return narrow(jnp.concatenate((gate_grad, up_grad), axis=1))


def ring_sum(terms):
    far_t, far_b, right_t, right_b, left_t, left_b, own_t, own_b = terms
    far_t = shift(far_t, "y", 1)
    far_b = shift(far_b, "y", -1)
    right_b = shift(right_b, "y", 1)
    left_t = shift(left_t, "y", -1)
    right_t = shift(narrow(right_t + far_t), "y", 1)
    left_b = shift(narrow(left_b + far_b), "y", -1)
    top = local_grads(own_t + left_t + right_t)
    low = local_grads(own_b + right_b + left_b)
    return top, low


def finish(place, grads, gates, ups, k):
    top, low = grads
    from_left_t = shift(top, "y", 1)
    from_right_b = shift(low, "y", -1)
    from_left_b = shift(low, "y", 1)
    from_right_t = shift(top, "y", -1)
    far_top = shift(from_left_t, "y", 1)
    far_low = shift(from_right_b, "y", -1)
    pieces = (far_top, far_low, from_right_t, from_right_b, from_left_t, from_left_b, top, low)
    partial_value = back_terms(place, pieces, gates, ups)
    blocks = partial_value.reshape(RING * RING, CHUNKS[k], -1)
    crossed = lax.all_to_all(blocks, XZ, 0, 0)
    return narrow(crossed.astype(jnp.float32).sum(axis=0))


def swap(value):
    return lax.ppermute(value, "core", [(0, 1), (1, 0)])


def step_shards(inputs, out_grad, gate_weight, up_weight, down_weight):
    gates = (gate_weight, swap(gate_weight))
    ups = (up_weight, swap(up_weight))
    downs = (down_weight, swap(down_weight))
    place = (lax.axis_index("y") + jnp.array(ORDER, jnp.int32)) % RING
    some_in = join("z", around(inputs, "z"))
    some_grad = join("x", around(out_grad, "x"))
    results = []
    terms = grads = None
    for k in range(len(CHUNKS)):
        in_pieces = around(some_in[k], "x")
        grad_pieces = around(some_grad[k], "z")
        if terms is not None:
            sums = ring_sum(terms)
        if terms is not None:
            results.append(finish(place, sums, gates, ups, k - 1))
        terms = pair_terms(place, in_pieces, gates, ups)
        terms = hidden_terms(place, grad_pieces, downs, terms)
    results.append(finish(place, ring_sum(terms), gates, ups, k))
    return jnp.concatenate(results, axis=0)


def solution(mesh):
    fine = Mesh(mesh.devices.reshape(2, 4, 4, 2, 2), ("xl", "z", "y", "xh", "core"))
    tokens = ("xl", "z", "xh", "core")
    return jax.shard_map(
        step_shards,
        mesh=fine,
        in_specs=(P(tokens, "y"), P(tokens, "y"), P("y", tokens), P("y", tokens), P(tokens, "y")),
        out_specs=P(tokens, "y"),
        check_vma=False,
    )
```

```python
import functools

import jax
import jax.numpy as jnp
from jax import lax
from jax.experimental import pallas as pl
from jax.experimental.pallas import tpu as pltpu
from jax.sharding import Mesh, PartitionSpec as P

CHUNKS = (40, 40)
RING = 4
XZ = ("xh", "xl", "z")
ORDER = (2, 1, 3, 0)
STEPS = (0, 1, 3, 2)
LAST = (((1,), (1,)), ((), ()))
VMEM_LIMIT = 46 << 20


def place_of(axis):
    if axis == "x":
        return lax.axis_index("xh") * 2 + lax.axis_index("xl")
    return lax.axis_index(axis)


def shift(value, axis, step):
    if axis == "x":
        order = lambda i: (i % 2) * 2 + i // 2
        pairs = [(order(i), order((i + step) % RING)) for i in range(RING)]
        return lax.ppermute(value, ("xl", "xh"), pairs)
    return lax.ppermute(value, axis, [(i, (i + step) % RING) for i in range(RING)])


def around(value, axis):
    return [value] + [shift(value, axis, step) for step in STEPS[1:]]


def join_kernel(rows, *refs):
    pieces, outs = refs[:RING], refs[RING:]
    for k in range(RING):
        at = 0
        for count, out in zip(rows, outs):
            out[k * count : (k + 1) * count] = pieces[k][at : at + count]
            at += count


def join(pieces):
    width = pieces[0].shape[1]
    spec = pl.BlockSpec(memory_space=pltpu.VMEM)
    return pl.pallas_call(
        functools.partial(join_kernel, CHUNKS),
        in_specs=[spec] * RING,
        out_specs=[spec] * len(CHUNKS),
        out_shape=[jax.ShapeDtypeStruct((RING * rows, width), pieces[0].dtype) for rows in CHUNKS],
        cost_estimate=pl.CostEstimate(flops=1 << 20, bytes_accessed=3 << 20, transcendentals=0),
        compiler_params=pltpu.CompilerParams(vmem_limit_bytes=16 << 20),
        name="join",
    )(*pieces)


def assemble(pieces, held):
    count = pieces[0].shape[0]
    for k, piece in enumerate(pieces):
        held[k * count : (k + 1) * count] = piece[...]


def pair_kernel(place, *refs, count, sides):
    pieces, (gate_a, gate_b, up_a, up_b) = refs[:count], refs[count : count + 4]
    outs, held = refs[-1 - RING * len(sides) : -1], refs[-1]
    step = pl.program_id(0)

    @pl.when(step == 0)
    def _():
        assemble(pieces, held)

    cols = jnp.concatenate((gate_a[...], gate_b[...], up_a[...], up_b[...]), axis=1)
    pair = jnp.dot(held[...], cols, preferred_element_type=jnp.float32)
    for k in range(RING):

        @pl.when(step == k)
        def _(k=k):
            at = 0
            for n in range(len(sides)):
                out = outs[len(sides) * k + n]
                out[...] = pair[at : at + out.shape[0]].astype(out.dtype)
                at += out.shape[0]


def pair_terms(place, pieces, gates, ups, first, terms):
    block, width = pieces[0].shape
    count = len(pieces)
    cut = gates[0].shape[1] // RING
    wide = 2 * cut
    bf, f32 = jnp.bfloat16, jnp.float32
    types = (bf, bf, f32, bf, bf, f32, f32, f32)
    sides, specs = [], []
    for side in range(2):
        low, high = max(first, 2 * side), min(first + count, 2 * side + 2)
        if low < high:
            sides.append(side)
            index = (low - 2 * side) // (high - low)
            specs.append(pl.BlockSpec(((high - low) * block, 2 * wide), lambda *_, i=index: (i, 0)))
    touched = [2 * k + side for k in range(RING) for side in sides]
    old = [] if terms is None else [terms[k] for k in touched]
    cols = pl.BlockSpec((width, cut), lambda step, place: (0, place[step]))
    grid_spec = pltpu.PrefetchScalarGridSpec(
        num_scalar_prefetch=1,
        grid=(RING,),
        in_specs=[pl.BlockSpec(memory_space=pltpu.VMEM)] * count
        + [cols] * 4
        + [pl.BlockSpec(memory_space=pl.ANY) for _ in old],
        out_specs=specs * RING,
        scratch_shapes=[pltpu.VMEM((count * block, width), bf)],
    )
    new = pl.pallas_call(
        functools.partial(pair_kernel, count=count, sides=tuple(sides)),
        grid_spec=grid_spec,
        out_shape=[jax.ShapeDtypeStruct((2 * block, 3 * wide), types[k]) for k in touched],
        input_output_aliases={1 + count + 4 + k: k for k in range(len(old))},
        cost_estimate=pl.CostEstimate(
            flops=2 * count * block * width * 8 * wide, bytes_accessed=14 << 20, transcendentals=0
        ),
        compiler_params=pltpu.CompilerParams(vmem_limit_bytes=VMEM_LIMIT),
        name="pair",
    )(place, *pieces, *gates, *ups, *old)
    if terms is None:
        return new
    terms = list(terms)
    for k, value in zip(touched, new):
        terms[k] = value
    return terms


def hidden_kernel(place, *refs):
    pieces, (down_a, down_b) = refs[:RING], refs[RING : RING + 2]
    refs, held = refs[RING + 2 : -1], refs[-1]
    outs = refs[len(refs) // 2 :]
    step = pl.program_id(0)
    half = outs[0].shape[0]
    count = half // (2 * RING)

    @pl.when(step == 0)
    def _():
        assemble(pieces, held)

    lines = jnp.concatenate((down_a[...], down_b[...]), axis=0)
    back = lax.dot_general(held[...], lines, LAST, preferred_element_type=jnp.float32)
    for k in range(len(outs) // 2):

        @pl.when(step == k)
        def _(k=k):
            for x in range(RING):
                out = outs[2 * k + x // 2]
                for z in range(RING):
                    to, at = ((x % 2) * RING + z) * count, (z * RING + x) * count
                    out[to : to + count] = back[at : at + count].astype(out.dtype)


def hidden_terms(place, pieces, downs, terms, first):
    rows, width = pieces[0].shape[0] * RING, pieces[0].shape[1]
    half = rows // 2
    steps = len(terms) // 2
    cut = downs[0].shape[0] // RING
    wide = 2 * cut
    lines = pl.BlockSpec((cut, width), lambda step, place: (place[step + first], 0))
    grid_spec = pltpu.PrefetchScalarGridSpec(
        num_scalar_prefetch=1,
        grid=(steps,),
        in_specs=[pl.BlockSpec(memory_space=pltpu.VMEM)] * RING
        + [lines, lines]
        + [pl.BlockSpec(memory_space=pl.ANY) for _ in terms],
        out_specs=[pl.BlockSpec((half, wide), lambda *_: (0, 2)) for _ in terms],
        scratch_shapes=[pltpu.VMEM((rows, width), jnp.bfloat16)],
    )
    return pl.pallas_call(
        hidden_kernel,
        grid_spec=grid_spec,
        out_shape=[jax.ShapeDtypeStruct(t.shape, t.dtype) for t in terms],
        input_output_aliases={1 + RING + 2 + k: k for k in range(2 * steps)},
        cost_estimate=pl.CostEstimate(
            flops=2 * rows * width * steps * wide, bytes_accessed=7 << 20, transcendentals=0
        ),
        compiler_params=pltpu.CompilerParams(vmem_limit_bytes=VMEM_LIMIT),
        name="hidden",
    )(place, *pieces, *downs, *terms)


def back_kernel(place, target, *rest):
    pieces, cols, out_ref, held = rest[:8], rest[8:12], rest[12], rest[13]
    half = pieces[0].shape[0]
    cut = pieces[0].shape[1] // 4
    span = RING * cut

    @pl.when(pl.program_id(0) == 0)
    def _():
        for k in range(RING):
            at = pl.multiple_of(place[k] * cut, cut)
            for side in range(2):
                for part in range(4):
                    held[side * half : (side + 1) * half, pl.ds(at + part * span, cut)] = pieces[
                        2 * k + side
                    ][:, part * cut : (part + 1) * cut]

    total = lax.dot_general(
        held[...],
        jnp.concatenate([c[...] for c in cols], axis=1),
        LAST,
        preferred_element_type=jnp.float32,
    )
    count = out_ref.shape[1]
    for k in range(RING * RING):
        out_ref[target[k]] = total[k * count : (k + 1) * count].astype(out_ref.dtype)


def back_terms(place, pieces, gates, ups, rows_cut=512):
    half = pieces[0].shape[0]
    width, span = gates[0].shape
    count = 2 * half // (RING * RING)
    steps = jnp.array(STEPS, jnp.int32)
    x = (place_of("x") - steps) % RING
    z = (place_of("z") - steps) % RING
    target = (x[:, None] * RING + z[None, :]).reshape(-1)
    grid_spec = pltpu.PrefetchScalarGridSpec(
        num_scalar_prefetch=2,
        grid=(width // rows_cut,),
        in_specs=[pl.BlockSpec(memory_space=pltpu.VMEM) for _ in pieces]
        + [pl.BlockSpec((rows_cut, span), lambda n, *_: (n, 0)) for _ in range(4)],
        out_specs=pl.BlockSpec((RING * RING, count, rows_cut), lambda n, *_: (0, 0, n)),
        scratch_shapes=[pltpu.VMEM((2 * half, 4 * span), jnp.bfloat16)],
    )
    return pl.pallas_call(
        back_kernel,
        grid_spec=grid_spec,
        out_shape=jax.ShapeDtypeStruct((RING * RING, count, width), jnp.bfloat16),
        cost_estimate=pl.CostEstimate(
            flops=16 * half * width * span, bytes_accessed=14 << 20, transcendentals=0
        ),
        compiler_params=pltpu.CompilerParams(vmem_limit_bytes=VMEM_LIMIT),
        name="back",
    )(place, target, *pieces, *gates, *ups)


def narrow(value):
    return value.astype(jnp.bfloat16)


def local_grads(total):
    wide = total.shape[1] // 3
    gate, upper, hidden_grad = total[:, :wide], total[:, wide : 2 * wide], total[:, 2 * wide :]
    logistic = jax.nn.sigmoid(gate)
    gate_grad = hidden_grad * upper * logistic * (1.0 + gate * (1.0 - logistic))
    up_grad = hidden_grad * gate * logistic
    return narrow(jnp.concatenate((gate_grad, up_grad), axis=1))


def ring_sum(terms):
    far_t, far_b, right_t, right_b, left_t, left_b, own_t, own_b = terms
    far_t = shift(far_t, "y", 1)
    far_b = shift(far_b, "y", -1)
    right_b = shift(right_b, "y", 1)
    left_t = shift(left_t, "y", -1)
    right_t = shift(narrow(right_t + far_t), "y", 1)
    left_b = shift(narrow(left_b + far_b), "y", -1)
    top = local_grads(own_t + left_t + right_t)
    low = local_grads(own_b + right_b + left_b)
    return top, low


def finish(place, grads, gates, ups):
    top, low = grads
    from_left_t = shift(top, "y", 1)
    from_right_b = shift(low, "y", -1)
    from_left_b = shift(low, "y", 1)
    from_right_t = shift(top, "y", -1)
    far_top = shift(from_left_t, "y", 1)
    far_low = shift(from_right_b, "y", -1)
    pieces = (far_top, far_low, from_right_t, from_right_b, from_left_t, from_left_b, top, low)
    partial_value = back_terms(place, pieces, gates, ups)
    crossed = lax.all_to_all(partial_value, XZ, 0, 0)
    return narrow(crossed.astype(jnp.float32).sum(axis=0))


def swap(value):
    return lax.ppermute(value, "core", [(0, 1), (1, 0)])


def step_shards(inputs, out_grad, gate_weight, up_weight, down_weight):
    gates = (gate_weight, swap(gate_weight))
    ups = (up_weight, swap(up_weight))
    downs = (down_weight, swap(down_weight))
    place = (lax.axis_index("y") + jnp.array(ORDER, jnp.int32)) % RING
    some_in = join(around(inputs, "z"))
    some_grad = join(around(out_grad, "x"))
    results = []
    terms = grads = None
    for k in range(len(CHUNKS)):
        in_pieces = around(some_in[k], "x")
        grad_pieces = around(some_grad[k], "z")
        if terms is not None:
            sums = ring_sum(terms)
        if terms is not None:
            results.append(finish(place, sums, gates, ups))
        if k:
            terms = pair_terms(place, in_pieces, gates, ups, 0, None)
        else:
            terms = pair_terms(place, in_pieces[:3], gates, ups, 0, None)
            terms = pair_terms(place, in_pieces[3:], gates, ups, 3, terms)
        far = hidden_terms(place, grad_pieces, downs, terms[:2], 0)
        near = hidden_terms(place, grad_pieces, downs, terms[2:], 1)
        terms = [*far, *near]
    results.append(finish(place, ring_sum(terms), gates, ups))
    return jnp.concatenate(results, axis=0)


def solution(mesh):
    fine = Mesh(mesh.devices.reshape(2, 4, 4, 2, 2), ("xl", "z", "y", "xh", "core"))
    tokens = ("xl", "z", "xh", "core")
    return jax.shard_map(
        step_shards,
        mesh=fine,
        in_specs=(P(tokens, "y"), P(tokens, "y"), P("y", tokens), P("y", tokens), P(tokens, "y")),
        out_specs=P(tokens, "y"),
        check_vma=False,
    )
```

```python
import functools

import jax
import jax.numpy as jnp
from jax import lax
from jax.experimental import pallas as pl
from jax.experimental.pallas import tpu as pltpu
from jax.sharding import Mesh, PartitionSpec as P

CHUNKS = (40, 40)
RING = 4
XZ = ("xh", "xl", "z")
ORDER = (2, 1, 3, 0)
STEPS = (0, 1, 3, 2)
LAST = (((1,), (1,)), ((), ()))
VMEM_LIMIT = 46 << 20


def place_of(axis):
    if axis == "x":
        return lax.axis_index("xh") * 2 + lax.axis_index("xl")
    return lax.axis_index(axis)


def shift(value, axis, step):
    if axis == "x":
        order = lambda i: (i % 2) * 2 + i // 2
        pairs = [(order(i), order((i + step) % RING)) for i in range(RING)]
        return lax.ppermute(value, ("xl", "xh"), pairs)
    return lax.ppermute(value, axis, [(i, (i + step) % RING) for i in range(RING)])


def around(value, axis):
    return [value] + [shift(value, axis, step) for step in STEPS[1:]]


def join_kernel(rows, own, *refs):
    pieces, outs, sems = refs[: RING - 1], refs[RING - 1 : -1], refs[-1]
    copies = []
    at = 0
    for n, (count, out) in enumerate(zip(rows, outs)):
        copies.append(
            pltpu.make_async_copy(own.at[pl.ds(at, count)], out.at[pl.ds(0, count)], sems.at[n])
        )
        copies[-1].start()
        at += count
    for k in range(1, RING):
        at = 0
        for count, out in zip(rows, outs):
            out[k * count : (k + 1) * count] = pieces[k - 1][at : at + count]
            at += count
    for copy in copies:
        copy.wait()


def join(pieces):
    width = pieces[0].shape[1]
    spec = pl.BlockSpec(memory_space=pltpu.VMEM)
    return pl.pallas_call(
        functools.partial(join_kernel, CHUNKS),
        in_specs=[pl.BlockSpec(memory_space=pl.ANY)] + [spec] * (RING - 1),
        out_specs=[spec] * len(CHUNKS),
        scratch_shapes=[pltpu.SemaphoreType.DMA((len(CHUNKS),))],
        out_shape=[jax.ShapeDtypeStruct((RING * rows, width), pieces[0].dtype) for rows in CHUNKS],
        cost_estimate=pl.CostEstimate(flops=1 << 20, bytes_accessed=3 << 20, transcendentals=0),
        compiler_params=pltpu.CompilerParams(vmem_limit_bytes=16 << 20),
        name="join",
    )(*pieces)


def assemble(pieces, held):
    count = pieces[0].shape[0]
    for k, piece in enumerate(pieces):
        held[k * count : (k + 1) * count] = piece[...]


def pair_kernel(place, *refs, count, sides):
    pieces, (gate_a, gate_b, up_a, up_b) = refs[:count], refs[count : count + 4]
    outs, held = refs[-1 - RING * len(sides) : -1], refs[-1]
    step = pl.program_id(0)

    @pl.when(step == 0)
    def _():
        assemble(pieces, held)

    cols = jnp.concatenate((gate_a[...], gate_b[...], up_a[...], up_b[...]), axis=1)
    pair = jnp.dot(held[...], cols, preferred_element_type=jnp.float32)
    for k in range(RING):

        @pl.when(step == k)
        def _(k=k):
            at = 0
            for n in range(len(sides)):
                out = outs[len(sides) * k + n]
                out[...] = pair[at : at + out.shape[0]].astype(out.dtype)
                at += out.shape[0]


def pair_terms(place, pieces, gates, ups, first, terms):
    block, width = pieces[0].shape
    count = len(pieces)
    cut = gates[0].shape[1] // RING
    wide = 2 * cut
    bf, f32 = jnp.bfloat16, jnp.float32
    types = (bf, bf, f32, bf, bf, f32, f32, f32)
    sides, specs = [], []
    for side in range(2):
        low, high = max(first, 2 * side), min(first + count, 2 * side + 2)
        if low < high:
            sides.append(side)
            index = (low - 2 * side) // (high - low)
            specs.append(pl.BlockSpec(((high - low) * block, 2 * wide), lambda *_, i=index: (i, 0)))
    touched = [2 * k + side for k in range(RING) for side in sides]
    old = [] if terms is None else [terms[k] for k in touched]
    cols = pl.BlockSpec((width, cut), lambda step, place: (0, place[step]))
    grid_spec = pltpu.PrefetchScalarGridSpec(
        num_scalar_prefetch=1,
        grid=(RING,),
        in_specs=[pl.BlockSpec(memory_space=pltpu.VMEM)] * count
        + [cols] * 4
        + [pl.BlockSpec(memory_space=pl.ANY) for _ in old],
        out_specs=specs * RING,
        scratch_shapes=[pltpu.VMEM((count * block, width), bf)],
    )
    new = pl.pallas_call(
        functools.partial(pair_kernel, count=count, sides=tuple(sides)),
        grid_spec=grid_spec,
        out_shape=[jax.ShapeDtypeStruct((2 * block, 3 * wide), types[k]) for k in touched],
        input_output_aliases={1 + count + 4 + k: k for k in range(len(old))},
        cost_estimate=pl.CostEstimate(
            flops=2 * count * block * width * 8 * wide, bytes_accessed=14 << 20, transcendentals=0
        ),
        compiler_params=pltpu.CompilerParams(vmem_limit_bytes=VMEM_LIMIT),
        name="pair",
    )(place, *pieces, *gates, *ups, *old)
    if terms is None:
        return new
    terms = list(terms)
    for k, value in zip(touched, new):
        terms[k] = value
    return terms


def hidden_kernel(place, *refs):
    pieces, (down_a, down_b) = refs[:RING], refs[RING : RING + 2]
    refs, held = refs[RING + 2 : -1], refs[-1]
    outs = refs[len(refs) // 2 :]
    step = pl.program_id(0)
    half = outs[0].shape[0]
    count = half // (2 * RING)

    @pl.when(step == 0)
    def _():
        assemble(pieces, held)

    lines = jnp.concatenate((down_a[...], down_b[...]), axis=0)
    back = lax.dot_general(held[...], lines, LAST, preferred_element_type=jnp.float32)
    for k in range(len(outs) // 2):

        @pl.when(step == k)
        def _(k=k):
            for x in range(RING):
                out = outs[2 * k + x // 2]
                for z in range(RING):
                    to, at = ((x % 2) * RING + z) * count, (z * RING + x) * count
                    out[to : to + count] = back[at : at + count].astype(out.dtype)


def hidden_terms(place, pieces, downs, terms, first):
    rows, width = pieces[0].shape[0] * RING, pieces[0].shape[1]
    half = rows // 2
    steps = len(terms) // 2
    cut = downs[0].shape[0] // RING
    wide = 2 * cut
    lines = pl.BlockSpec((cut, width), lambda step, place: (place[step + first], 0))
    grid_spec = pltpu.PrefetchScalarGridSpec(
        num_scalar_prefetch=1,
        grid=(steps,),
        in_specs=[pl.BlockSpec(memory_space=pltpu.VMEM)] * RING
        + [lines, lines]
        + [pl.BlockSpec(memory_space=pl.ANY) for _ in terms],
        out_specs=[pl.BlockSpec((half, wide), lambda *_: (0, 2)) for _ in terms],
        scratch_shapes=[pltpu.VMEM((rows, width), jnp.bfloat16)],
    )
    return pl.pallas_call(
        hidden_kernel,
        grid_spec=grid_spec,
        out_shape=[jax.ShapeDtypeStruct(t.shape, t.dtype) for t in terms],
        input_output_aliases={1 + RING + 2 + k: k for k in range(2 * steps)},
        cost_estimate=pl.CostEstimate(
            flops=2 * rows * width * steps * wide, bytes_accessed=7 << 20, transcendentals=0
        ),
        compiler_params=pltpu.CompilerParams(vmem_limit_bytes=VMEM_LIMIT),
        name="hidden",
    )(place, *pieces, *downs, *terms)


def back_kernel(place, target, *rest):
    pieces, cols, out_ref, held = rest[:8], rest[8:12], rest[12], rest[13]
    half = pieces[0].shape[0]
    cut = pieces[0].shape[1] // 4
    span = RING * cut

    @pl.when(pl.program_id(0) == 0)
    def _():
        for k in range(RING):
            at = pl.multiple_of(place[k] * cut, cut)
            for side in range(2):
                for part in range(4):
                    held[side * half : (side + 1) * half, pl.ds(at + part * span, cut)] = pieces[
                        2 * k + side
                    ][:, part * cut : (part + 1) * cut]

    total = lax.dot_general(
        held[...],
        jnp.concatenate([c[...] for c in cols], axis=1),
        LAST,
        preferred_element_type=jnp.float32,
    )
    count = out_ref.shape[1]
    for k in range(RING * RING):
        out_ref[target[k]] = total[k * count : (k + 1) * count].astype(out_ref.dtype)


def back_terms(place, pieces, gates, ups, rows_cut=512):
    half = pieces[0].shape[0]
    width, span = gates[0].shape
    count = 2 * half // (RING * RING)
    steps = jnp.array(STEPS, jnp.int32)
    x = (place_of("x") - steps) % RING
    z = (place_of("z") - steps) % RING
    target = (x[:, None] * RING + z[None, :]).reshape(-1)
    grid_spec = pltpu.PrefetchScalarGridSpec(
        num_scalar_prefetch=2,
        grid=(width // rows_cut,),
        in_specs=[pl.BlockSpec(memory_space=pltpu.VMEM) for _ in pieces]
        + [pl.BlockSpec((rows_cut, span), lambda n, *_: (n, 0)) for _ in range(4)],
        out_specs=pl.BlockSpec((RING * RING, count, rows_cut), lambda n, *_: (0, 0, n)),
        scratch_shapes=[pltpu.VMEM((2 * half, 4 * span), jnp.bfloat16)],
    )
    return pl.pallas_call(
        back_kernel,
        grid_spec=grid_spec,
        out_shape=jax.ShapeDtypeStruct((RING * RING, count, width), jnp.bfloat16),
        cost_estimate=pl.CostEstimate(
            flops=16 * half * width * span, bytes_accessed=14 << 20, transcendentals=0
        ),
        compiler_params=pltpu.CompilerParams(vmem_limit_bytes=30 << 20),
        name="back",
    )(place, target, *pieces, *gates, *ups)


def narrow(value):
    return value.astype(jnp.bfloat16)


def local_grads(total):
    wide = total.shape[1] // 3
    gate, upper, hidden_grad = total[:, :wide], total[:, wide : 2 * wide], total[:, 2 * wide :]
    logistic = jax.nn.sigmoid(gate)
    gate_grad = hidden_grad * upper * logistic * (1.0 + gate * (1.0 - logistic))
    up_grad = hidden_grad * gate * logistic
    return narrow(jnp.concatenate((gate_grad, up_grad), axis=1))


def ring_sum(terms):
    far_t, far_b, right_t, right_b, left_t, left_b, own_t, own_b = terms
    far_t = shift(far_t, "y", 1)
    far_b = shift(far_b, "y", -1)
    right_b = shift(right_b, "y", 1)
    left_t = shift(left_t, "y", -1)
    right_t = shift(narrow(right_t + far_t), "y", 1)
    left_b = shift(narrow(left_b + far_b), "y", -1)
    top = local_grads(own_t + left_t + right_t)
    low = local_grads(own_b + right_b + left_b)
    return top, low


def finish(place, grads, gates, ups):
    top, low = grads
    from_left_t = shift(top, "y", 1)
    from_right_b = shift(low, "y", -1)
    from_left_b = shift(low, "y", 1)
    from_right_t = shift(top, "y", -1)
    far_top = shift(from_left_t, "y", 1)
    far_low = shift(from_right_b, "y", -1)
    pieces = (far_top, far_low, from_right_t, from_right_b, from_left_t, from_left_b, top, low)
    partial_value = back_terms(place, pieces, gates, ups)
    crossed = lax.all_to_all(partial_value, XZ, 0, 0)
    return narrow(crossed.astype(jnp.float32).sum(axis=0))


def swap(value):
    return lax.ppermute(value, "core", [(0, 1), (1, 0)])


def step_shards(inputs, out_grad, gate_weight, up_weight, down_weight):
    gates = (gate_weight, swap(gate_weight))
    ups = (up_weight, swap(up_weight))
    downs = (down_weight, swap(down_weight))
    place = (lax.axis_index("y") + jnp.array(ORDER, jnp.int32)) % RING
    some_in = join(around(inputs, "z"))
    some_grad = join(around(out_grad, "x"))
    results = []
    terms = grads = None
    for k in range(len(CHUNKS)):
        in_pieces = around(some_in[k], "x")
        grad_pieces = around(some_grad[k], "z")
        if terms is not None:
            sums = ring_sum(terms)
        if terms is not None:
            results.append(finish(place, sums, gates, ups))
        if k:
            terms = pair_terms(place, in_pieces, gates, ups, 0, None)
        else:
            terms = pair_terms(place, in_pieces[:3], gates, ups, 0, None)
            terms = pair_terms(place, in_pieces[3:], gates, ups, 3, terms)
        far = hidden_terms(place, grad_pieces, downs, terms[:2], 0)
        near = hidden_terms(place, grad_pieces, downs, terms[2:], 1)
        terms = [*far, *near]
    results.append(finish(place, ring_sum(terms), gates, ups))
    return jnp.concatenate(results, axis=0)


def solution(mesh):
    fine = Mesh(mesh.devices.reshape(2, 4, 4, 2, 2), ("xl", "z", "y", "xh", "core"))
    tokens = ("xl", "z", "xh", "core")
    return jax.shard_map(
        step_shards,
        mesh=fine,
        in_specs=(P(tokens, "y"), P(tokens, "y"), P("y", tokens), P("y", tokens), P(tokens, "y")),
        out_specs=P(tokens, "y"),
        check_vma=False,
    )
```
